512 devices in a mesh: cfg: 2 (over y), site: 16 (over z), vec: 8 (over x), tslice: 2 (over core).
Axes of the slice: x: 8, y: 2, z: 16, core: 2. Of those that a mesh axis runs over, the one named last changes fastest.
The devices are a block of a 8x8x16 slice.
Arguments:
- eigvecs: float32 [4, 2, 3, 384, 16, 512], P(('cfg', 'tslice'), None, None, 'vec', 'site'), parts along dimension 0, may hold values from -1 to 1
- links: float32 [4, 3, 2, 3, 3, 16, 512], P(('cfg', 'tslice'), None, None, None, None, 'site'), parts along dimension 0, may hold values from -1 to 1, as said below
- peramb: bfloat16 [4, 32, 4, 2, 384, 384], P(('cfg', 'tslice'), 'site', None, None, 'vec'), parts along dimension 0, may hold values from -0.21875 to 0.21875
- block_owner: int32 [8], replicated, may hold values from 0 to 7, each once
- momenta: int32 [2, 3], replicated, may hold values from -2 to 2, as said below
Outputs:
- projected: bfloat16 [4, 32, 4, 2, 2, 384, 384], P(('cfg', 'tslice'), 'site', None, None, None, 'vec'), parts along dimension 0
The draws below stay inside these ranges and needn't reach their ends.
There are 2 independent parts, one for each index of `cfg`. The reference program is written for one: setup_inputs(seed, part) draws one part's arguments, and reference() takes and returns one part's arrays. A program takes and returns all parts, laid end to end along the dimension named above; an argument that names none is the same for every part. Nothing has to cross between parts.
Inputs may be any that keep to these rules, and one draw needn't show every extreme that they name: Block b of eigvecs holds the eigenvectors numbered from block_owner[b] * 48 on; every block number appears once. `momenta`: every component is -2, -1, 1 or 2, never zero. `links`: every 3 x 3 link matrix is unitary.
All inputs are finite; a program needn't handle non-finite values.
Results may differ from the reference program's by a relative error of at most 0.0065.
Values may be sent and summed in bfloat16 or wider, within the bound.
A program may use at most 64 MiB of HBM per device.

```python
import math
import jax
import jax.numpy as jnp
from jax import lax

NVEC = 384
LX = 32
LY = 16
K = 2
P_SIZE = 2
SPINS = 4
LZ = 16
LXY = 512
NT = 2
NSINK = 32
NBLK = 8


def draw_momenta(key, part):
    raw = jax.random.randint(jax.random.fold_in(key, 11), (P_SIZE, 3), 0, 4, dtype=jnp.int32)
    return raw - 2 + (raw >= 2).astype(jnp.int32)


def complex_product(left_re, left_im, right_re, right_im):
    out_re = []
    out_im = []
    for row in range(3):
        line_re = []
        line_im = []
        for col in range(3):
            acc_re = left_re[row][0] * right_re[0][col] - left_im[row][0] * right_im[0][col]
            acc_im = left_re[row][0] * right_im[0][col] + left_im[row][0] * right_re[0][col]
            for mid in range(1, 3):
                acc_re = acc_re + left_re[row][mid] * right_re[mid][col] - left_im[row][mid] * right_im[mid][col]
                acc_im = acc_im + left_re[row][mid] * right_im[mid][col] + left_im[row][mid] * right_re[mid][col]
            line_re.append(acc_re)
            line_im.append(acc_im)
        out_re.append(line_re)
        out_im.append(line_im)
    return (out_re, out_im)


def givens(first, second, rotation, phase_a, phase_b):
    zeros = jnp.zeros_like(rotation)
    ones = jnp.ones_like(rotation)
    mat_re = [[ones if r == c else zeros for c in range(3)] for r in range(3)]
    mat_im = [[zeros for c in range(3)] for r in range(3)]
    cosine = jnp.cos(rotation)
    sine = jnp.sin(rotation)
    mat_re[first][first] = cosine * jnp.cos(phase_a)
    mat_im[first][first] = cosine * jnp.sin(phase_a)
    mat_re[first][second] = sine * jnp.cos(phase_b)
    mat_im[first][second] = sine * jnp.sin(phase_b)
    mat_re[second][first] = -sine * jnp.cos(phase_b)
    mat_im[second][first] = sine * jnp.sin(phase_b)
    mat_re[second][second] = cosine * jnp.cos(phase_a)
    mat_im[second][second] = -cosine * jnp.sin(phase_a)
    return (mat_re, mat_im)


def draw_links(key, part):
    shape = (12, NT, 3, LZ, LX * LY)
    angles = jax.random.uniform(jax.random.fold_in(key, 23), shape, jnp.float32, -3.14159265, 3.14159265)
    zeros = jnp.zeros_like(angles[0])
    diag_re = [[jnp.cos(angles[r]) if r == c else zeros for c in range(3)] for r in range(3)]
    diag_im = [[jnp.sin(angles[r]) if r == c else zeros for c in range(3)] for r in range(3)]
    total_re, total_im = (diag_re, diag_im)
    pairs = [(0, 1), (1, 2), (0, 2)]
    for index in range(3):
        first, second = pairs[index]
        base = 3 + 3 * index
        rot_re, rot_im = givens(first, second, angles[base], angles[base + 1], angles[base + 2])
        total_re, total_im = complex_product(total_re, total_im, rot_re, rot_im)
    real = jnp.stack([jnp.stack(row, axis=2) for row in total_re], axis=2)
    imag = jnp.stack([jnp.stack(row, axis=2) for row in total_im], axis=2)
    return jnp.stack([real, imag], axis=2)


def steps_of(key, dims, shards, low, largest):
    level, own = 1.0, jax.random.fold_in(key, 6)
    for position, shards_of in shards:
        draws = jnp.exp(jax.random.uniform(jax.random.fold_in(own, position), (shards_of,), jnp.float32, low / len(shards), largest / len(shards)))
        level = level * jnp.repeat(draws, dims[position] // shards_of).reshape([-1 if axis == position else 1 for axis in range(len(dims))])
    return level


def normal_values(own_key, shape, spread, bound, split=(), kind=jnp.bfloat16):
    values = jax.random.normal(own_key, shape, jnp.float32) * spread
    if len(split) > 0:
        values = steps_of(own_key, shape, split, -0.22, 0.18) * values
    return jnp.clip(values, min=-bound, max=bound).astype(kind)


def setup_inputs(seed: int = 0, part: int = 0) -> dict:
    keys = jax.random.split(jax.random.key(seed), 6)
    part_splits = jax.random.split(jax.random.fold_in(keys[5], part), 6)
    eigvecs = normal_values(part_splits[0], (NT, 2, 3, NVEC, LZ, LXY), ((6 * LX * LY * LZ) ** -0.25), 1.0, ((0, 2), (3, 8), (4, 16)), jnp.float32)
    links = draw_links(jax.random.fold_in(jax.random.fold_in(keys[5], part), 71), part)
    peramb = normal_values(part_splits[2], (NT, NSINK, SPINS, 2, NVEC, NVEC), (2 * NVEC) ** -0.5, 0.21875, ((0, 2), (1, 16), (4, 8)))
    block_owner = jax.random.permutation(keys[3], NBLK).astype(jnp.int32)
    momenta = draw_momenta(jax.random.fold_in(keys[5], 71), part)
    return {"eigvecs": eigvecs, "links": links, "peramb": peramb, "block_owner": block_owner, "momenta": momenta}


two_pi = 2.0 * math.pi


def along(field, direction, sense):
    width = field.shape[-1]
    column = lax.broadcasted_iota(jnp.int32, (width,), 0) % LX
    if direction == 0:
        if sense > 0:
            return jnp.where(column == LX - 1, jnp.roll(field, LX - 1, -1), jnp.roll(field, -1, -1))
        return jnp.where(column == 0, jnp.roll(field, 1 - LX, -1), jnp.roll(field, 1, -1))
    return jnp.roll(field, -sense * LX, -1)


def link_times(link_re, link_im, field_re, field_im, dagger):
    result_re = []
    result_im = []
    for target in range(3):
        summed_re = jnp.zeros_like(field_re[0])
        summed_im = jnp.zeros_like(field_re[0])
        for source in range(3):
            if dagger:
                entry_re = link_re[source, target][None]
                entry_im = -link_im[source, target][None]
            else:
                entry_re = link_re[target, source][None]
                entry_im = link_im[target, source][None]
            summed_re = summed_re + entry_re * field_re[source] - entry_im * field_im[source]
            summed_im = summed_im + entry_re * field_im[source] + entry_im * field_re[source]
        result_re.append(summed_re)
        result_im.append(summed_im)
    return jnp.stack(result_re), jnp.stack(result_im)


def chebyshev(initial, operate):
    previous = initial
    current = operate(initial)
    for repeat in range(K - 1):
        following = 2.0 * operate(current) - previous
        previous = current
        current = following
    return current


def phase_angle(momenta, across, upward, depth, extent):
    return two_pi * ((momenta[:, 0, None, None] * across[None]).astype(jnp.float32) / LX
                     + (momenta[:, 1, None, None] * upward[None]).astype(jnp.float32) / LY
                     + (momenta[:, 2, None, None] * depth[None]).astype(jnp.float32) / extent)


def hop_full(field, links_slice):
    total_re = jnp.zeros_like(field[0])
    total_im = jnp.zeros_like(field[0])
    for direction in range(3):
        link_re = links_slice[direction, 0]
        link_im = links_slice[direction, 1]
        if direction < 2:
            ahead = along(field, direction, 1)
            behind = along(field, direction, -1)
            back_re = along(link_re, direction, -1)
            back_im = along(link_im, direction, -1)
        else:
            ahead = jnp.roll(field, -1, 3)
            behind = jnp.roll(field, 1, 3)
            back_re = jnp.roll(link_re, 1, 2)
            back_im = jnp.roll(link_im, 1, 2)
        forward = link_times(link_re, link_im, ahead[0], ahead[1], False)
        backward = link_times(back_re, back_im, behind[0], behind[1], True)
        total_re = total_re + forward[0] + backward[0]
        total_im = total_im + forward[1] + backward[1]
    return jnp.stack([total_re, total_im]) * (-1.0 / 6.0)


def reference(eigvecs, links, peramb, block_owner, momenta):
    block = NVEC // NBLK
    ranks = jnp.arange(NBLK, dtype=jnp.int32)
    inverse = jnp.sum(ranks[:, None] * (block_owner[:, None] == ranks[None, :]).astype(jnp.int32), axis=0)
    flat = lax.broadcasted_iota(jnp.int32, (LZ, LXY), 1)
    depth = lax.broadcasted_iota(jnp.int32, (LZ, LXY), 0)
    theta = phase_angle(momenta, flat % LX, flat // LX, depth, LZ)

    def one_slice(operands):
        vectors, links_slice, perambulator = operands
        grouped = vectors.reshape(2, 3, NBLK, block, LZ, LXY)
        ordered = jnp.take(grouped, inverse, axis=2)
        blocks_first = jnp.moveaxis(ordered, 2, 0)
        filtered_blocks = lax.map(lambda field: chebyshev(field, lambda source_field: hop_full(source_field, links_slice)), blocks_first)
        filtered = jnp.moveaxis(filtered_blocks, 0, 2).reshape(2, 3, NVEC, LZ, LXY).astype(jnp.bfloat16)
        left = filtered.astype(jnp.float32)

        def elemental(angle):
            cosine = jnp.cos(angle)
            sine = jnp.sin(angle)
            shift_re = cosine * left[0] + sine * left[1]
            shift_im = cosine * left[1] - sine * left[0]
            shifted = jnp.stack([shift_re, shift_im]).astype(jnp.bfloat16)
            shifted_values = lax.optimization_barrier(shifted).astype(jnp.float32)
            product = jnp.einsum("acizs,bckzs->aibk", left, shifted_values, precision=lax.Precision.HIGHEST)
            real = product[0, :, 0] + product[1, :, 1]
            imag = product[0, :, 1] - product[1, :, 0]
            return jnp.stack([real, imag])

        phi = lax.map(elemental, theta)
        phi_rounded = phi.astype(jnp.bfloat16)
        phi_values = lax.optimization_barrier(phi_rounded).astype(jnp.float32)

        def one_sink(tau):
            tau_values = tau.astype(jnp.float32)
            real = (jnp.einsum("qij,pjk->qpik", tau_values[:, 0], phi_values[:, 0], precision=lax.Precision.HIGHEST)
                    - jnp.einsum("qij,pjk->qpik", tau_values[:, 1], phi_values[:, 1], precision=lax.Precision.HIGHEST))
            imag = (jnp.einsum("qij,pjk->qpik", tau_values[:, 0], phi_values[:, 1], precision=lax.Precision.HIGHEST)
                    + jnp.einsum("qij,pjk->qpik", tau_values[:, 1], phi_values[:, 0], precision=lax.Precision.HIGHEST))
            return jnp.stack([real, imag], axis=2).astype(jnp.bfloat16)

        return lax.map(one_sink, perambulator)

    return lax.map(one_slice, (eigvecs, links, peramb))
```

```python
import functools
import math

import jax
import jax.numpy as jnp
from jax import lax
from jax.experimental import pallas as pl
from jax.experimental.pallas import tpu as pltpu
from jax.sharding import PartitionSpec as P

LX = 32
LY = 16
LANES = 128
ROWS = 16
MESH = pl.DeviceIdType.MESH
F32 = jnp.float32
BF16 = jnp.bfloat16

two_pi = 2.0 * math.pi

ORDER = (
    "f0 f1 F01 f2",
    "F02 F11 F03 F12",
    "F04 M0 F21 F13",
    "F22 F14 M1 F23",
    "R0 F24 M2 R1",
    "Z0 R2 X01 Z1",
    "X02 X11 Z2 X03",
    "X12 X21 X04 X13",
    "X22 X14 X23 X24",
)


def link_times(entry, re, im, dagger):
    out_re, out_im = [], []
    for target in range(3):
        total_re = total_im = None
        for source in range(3):
            place = source * 3 + target if dagger else target * 3 + source
            ere, eim = entry[place], entry[9 + place]
            if dagger:
                tre = ere * re[source] + eim * im[source]
                tim = ere * im[source] - eim * re[source]
            else:
                tre = ere * re[source] - eim * im[source]
                tim = ere * im[source] + eim * re[source]
            total_re = tre if total_re is None else total_re + tre
            total_im = tim if total_im is None else total_im + tim
        out_re.append(total_re)
        out_im.append(total_im)
    return out_re + out_im


def elementals(
    ring, sites, chunks, momenta_count,
    x0, links, owner, momenta, phi_out,
    shifted_links, lk, cs, t1, acc, raw0, back0, raw1, back1, above0, below0, above1, below1,
    weights, *rest,
):
    gathered, parts, rs_in, phi = (rest[k * chunks : (k + 1) * chunks] for k in range(4))
    halo_send, halo_recv, f_send, f_recv, rs_send, rs_recv, z_send, z_recv, x_send, x_recv = rest[4 * chunks :]
    x = lax.axis_index("vec")
    z = lax.axis_index("site")
    plane = links.shape[-1]
    tiles = plane // LANES
    block = chunks * ROWS
    half_ring = ring // 2
    groups = parts[0].shape[0]
    group_rows = parts[0].shape[1]

    barrier = pltpu.get_barrier_semaphore()

    def greet(d, carry):
        pl.semaphore_signal(barrier, inc=1, device_id={"site": lax.rem(z + d, sites)}, device_id_type=MESH)
        return carry

    lax.fori_loop(1, sites, greet, 0)
    for d in (1, ring - 1):
        pl.semaphore_signal(barrier, inc=1, device_id={"vec": lax.rem(x + d, ring)}, device_id_type=MESH)

    column = lax.broadcasted_iota(jnp.int32, (18, plane), 1) % LX
    link_x, link_y = links[0:18], links[18:36]
    shifted_links[0:18] = link_x
    shifted_links[18:36] = jnp.where(
        column == 0, pltpu.roll(link_x, plane + 1 - LX, 1), pltpu.roll(link_x, 1, 1)
    )
    shifted_links[36:54] = link_y
    shifted_links[54:72] = pltpu.roll(link_y, LX, 1)
    shifted_links[72:90] = links[36:54]

    def spread(e, carry):
        lk[e] = jnp.broadcast_to(shifted_links[pl.ds(e, 1), :], (8, plane))
        return carry

    lax.fori_loop(0, 90, spread, 0)

    flat = lax.broadcasted_iota(jnp.int32, (8, plane), 1)
    for p in range(momenta_count):
        theta = two_pi * (
            (momenta[p, 0] * (flat % LX)).astype(F32) / LX
            + (momenta[p, 1] * (flat // LX)).astype(F32) / LY
            + (jnp.zeros_like(flat) + momenta[p, 2] * z).astype(F32) / sites
        )
        cs[p, 0] = jnp.cos(theta)
        cs[p, 1] = jnp.sin(theta)

    def lanes_of(t):
        return pl.ds(pl.multiple_of(t * LANES, LANES), LANES)

    def entries(hop, lanes):
        return [lk[hop * 18 + e, :, lanes][None] for e in range(18)]

    def vectors(ref, c, lanes):
        return [ref[comp, pl.ds(2 * c, 2), :, lanes] for comp in range(6)]

    def pack(value):
        return value.reshape(ROWS, LANES).astype(BF16)

    def unpack(value):
        return value.astype(F32).reshape(2, 8, LANES)

    lane = lax.broadcasted_iota(jnp.int32, (2, 8, LANES), 2)
    last_column = lane % LX == LX - 1
    first_column = lane % LX == 0

    def roll(value, shift):
        return pltpu.roll(value.reshape(ROWS, LANES), shift, 1).reshape(2, 8, LANES)

    def outgoing(source, raw, back, c):
        def body(t, carry):
            lanes = lanes_of(t)
            field = vectors(source, c, lanes)
            sent = link_times(entries(4, lanes), field[:3], field[3:], True)
            for comp in range(6):
                raw[c, comp, :, lanes] = pack(field[comp])
                back[c, comp, :, lanes] = pack(sent[comp])
            return carry

        lax.fori_loop(0, tiles, body, 0)

    def in_plane(source, c):
        def body(t, carry):
            lanes = lanes_of(t)
            field = vectors(source, c, lanes)
            ahead = [jnp.where(last_column, roll(w, LX - 1), roll(w, LANES - 1)) for w in field]
            total = link_times(entries(0, lanes), ahead[:3], ahead[3:], False)
            behind = [jnp.where(first_column, roll(w, LANES + 1 - LX), roll(w, 1)) for w in field]
            added = link_times(entries(1, lanes), behind[:3], behind[3:], True)
            total = [a + b for a, b in zip(total, added)]
            after = vectors(source, c, lanes_of(lax.rem(t + 1, tiles)))
            ahead = [
                jnp.where(lane < LANES - LX, roll(w, LANES - LX), roll(v, LANES - LX)) for w, v in zip(field, after)
            ]
            added = link_times(entries(2, lanes), ahead[:3], ahead[3:], False)
            total = [a + b for a, b in zip(total, added)]
            before = vectors(source, c, lanes_of(lax.rem(t + tiles - 1, tiles)))
            behind = [jnp.where(lane >= LX, roll(w, LX), roll(v, LX)) for w, v in zip(field, before)]
            added = link_times(entries(3, lanes), behind[:3], behind[3:], True)
            for comp in range(6):
                acc[comp, pl.ds(2 * c, 2), :, lanes] = total[comp] + added[comp]
            return carry

        lax.fori_loop(0, tiles, body, 0)

    def applied(c, lanes, above, below):
        total = vectors(acc, c, lanes)
        field = [unpack(above[c, comp, :, lanes]) for comp in range(6)]
        added = link_times(entries(4, lanes), field[:3], field[3:], False)
        return [
            (total[comp] + added[comp] + unpack(below[c, comp, :, lanes])) * (-1.0 / 6.0) for comp in range(6)
        ]

    up, down = lax.rem(z + 1, sites), lax.rem(z + sites - 1, sites)
    started = []

    def halo(round_, c):
        raw, back, above, below = (raw0, back0, above0, below0) if round_ == 0 else (raw1, back1, above1, below1)
        return [
            pltpu.make_async_remote_copy(
                src_ref=raw.at[c], dst_ref=above.at[c],
                send_sem=halo_send.at[round_, 0, c], recv_sem=halo_recv.at[round_, 0, c],
                device_id={"site": down}, device_id_type=MESH,
            ),
            pltpu.make_async_remote_copy(
                src_ref=back.at[c], dst_ref=below.at[c],
                send_sem=halo_send.at[round_, 1, c], recv_sem=halo_recv.at[round_, 1, c],
                device_id={"site": up}, device_id_type=MESH,
            ),
        ]

    def send_halo(round_, c):
        for copy in halo(round_, c):
            copy.start()
            started.append(copy)

    def wait_halo(round_, c):
        for copy in halo(round_, c):
            copy.wait_recv()

    for c in range(chunks):
        outgoing(x0, raw0, back0, c)
    pl.semaphore_wait(barrier, sites - 1 + 2)
    for c in range(chunks):
        send_halo(0, c)
    for c in range(chunks):
        in_plane(x0, c)
    for c in range(chunks):
        wait_halo(0, c)

        def first(t, carry, c=c):
            lanes = lanes_of(t)
            result = applied(c, lanes, above0, below0)
            sent = link_times(entries(4, lanes), result[:3], result[3:], True)
            for comp in range(6):
                t1[comp, pl.ds(2 * c, 2), :, lanes] = result[comp]
                raw1[c, comp, :, lanes] = pack(result[comp])
                back1[c, comp, :, lanes] = pack(sent[comp])
            return carry

        lax.fori_loop(0, tiles, first, 0)
        send_halo(1, c)
        in_plane(t1, c)

    def ring_copy(buffers, span, sends, recvs, way, c, step, half, block_of):
        sign = 1 if way == 0 else ring - 1
        here = buffers[c].at[block_of, pl.ds(half * span, span)]
        return pltpu.make_async_remote_copy(
            src_ref=here, dst_ref=here,
            send_sem=sends.at[way, c, step - 1, half], recv_sem=recvs.at[way, c, step - 1, half],
            device_id={"vec": lax.rem(x + sign, ring)}, device_id_type=MESH,
        )

    def ring_send(buffers, span, sends, recvs, c, step, half, way):
        if step == half_ring and half != way:
            return
        back_by = (ring - (step - 1)) if way == 0 else (step - 1)
        copy = ring_copy(buffers, span, sends, recvs, way, c, step, half, lax.rem(x + back_by, ring))
        copy.start()
        started.append(copy)

    def ring_forward(buffers, span, sends, recvs, c, step):
        for half in range(2):
            for way in range(2):
                if step == half_ring and half != way:
                    continue
                back_by = (ring - step) if way == 0 else step
                ring_copy(
                    buffers, span, sends, recvs, way, c, step, half, lax.rem(x + back_by, ring)
                ).wait_recv()
                if step < half_ring:
                    ring_send(buffers, span, sends, recvs, c, step + 1, half, way)

    vectors_ring = (gathered, 3, f_send, f_recv)
    elemental_rows = phi[0].shape[1] // 2
    phi_ring = (phi, elemental_rows, x_send, x_recv)

    def start_ring(which, c):
        for half in range(2):
            for way in range(2):
                ring_send(*which, c, 1, half, way)

    def filter_chunk(c):
        wait_halo(1, c)

        def second(t, carry):
            lanes = lanes_of(t)
            result = applied(c, lanes, above1, below1)
            start = vectors(x0, c, lanes)
            for comp in range(6):
                gathered[c][x, comp, :, lanes] = pack(2.0 * result[comp] - start[comp])
            return carry

        lax.fori_loop(0, tiles, second, 0)
        start_ring(vectors_ring, c)

        def phases(t, carry):
            lanes = lanes_of(t)
            for color in range(3):
                re = unpack(gathered[c][x, color, :, lanes])
                im = unpack(gathered[c][x, 3 + color, :, lanes])
                for p in range(momenta_count):
                    cosine, sine = cs[p, 0, :, lanes][None], cs[p, 1, :, lanes][None]
                    shift_re = pack(cosine * re + sine * im)
                    shift_im = pack(cosine * im - sine * re)
                    real = pl.ds(2 * p * block + c * ROWS, ROWS)
                    imag = pl.ds((2 * p + 1) * block + c * ROWS, ROWS)
                    weights[color, real, lanes] = shift_re
                    weights[3 + color, real, lanes] = shift_im
                    weights[color, imag, lanes] = shift_im
                    weights[3 + color, imag, lanes] = -shift_re
            return carry

        lax.fori_loop(0, tiles, phases, 0)

    inverse = []
    for place in range(ring):
        found = 0
        for b in range(ring):
            found = jnp.where(owner[b] == place, b, found)
        inverse.append(found)

    def group_of(device):
        index = (device * groups + sites - 1) // sites
        return index, jnp.logical_and(index < groups, (index * sites) // groups == device)

    my_group, reduces = group_of(z)
    spare = jnp.where(reduces, my_group, 0)

    def far_first(i):
        k = (i + 1) // 2
        return sites // 2 + jnp.where(i % 2 == 0, k, -k)

    def partial_copy(c, group, target, source):
        return pltpu.make_async_remote_copy(
            src_ref=parts[c].at[group], dst_ref=rs_in[c].at[source],
            send_sem=rs_send.at[c, group], recv_sem=rs_recv.at[c, source],
            device_id={"site": target}, device_id_type=MESH,
        )

    def multiply(c):
        total = None
        for comp in range(6):
            left = weights[comp]
            right = jnp.concatenate([gathered[c][inverse[place], comp] for place in range(ring)], axis=0)
            product = lax.dot_general(left, right, (((1,), (1,)), ((), ())), preferred_element_type=F32)
            total = product if total is None else total + product
        parts[c][...] = total.reshape(groups, group_rows, ring * ROWS).astype(BF16)

        def send(i, carry):
            target = lax.rem(z + far_first(i), sites)
            group, valid = group_of(target)

            @pl.when(valid)
            def _():
                partial_copy(c, group, target, z).start()

            return carry

        lax.fori_loop(0, sites - 1, send, 0)

    def z_copy(c, group, target, number):
        rows = pl.ds(pl.multiple_of(group * group_rows, ROWS), group_rows)
        here = phi[c].at[x, rows]
        return pltpu.make_async_remote_copy(
            src_ref=here, dst_ref=here,
            send_sem=z_send.at[c, number], recv_sem=z_recv.at[c, group],
            device_id={"site": target}, device_id_type=MESH,
        )

    def reduce(c):
        @pl.when(reduces)
        def _():
            def arrive(i, carry):
                source = lax.rem(z + i, sites)
                partial_copy(c, spare, z, source).wait_recv()
                return carry

            lax.fori_loop(1, sites, arrive, 0)

            def add(i, total):
                return total + rs_in[c][lax.rem(z + i, sites)].astype(F32)

            total = lax.fori_loop(1, sites, add, parts[c][spare].astype(F32))
            rows = pl.ds(pl.multiple_of(spare * group_rows, ROWS), group_rows)
            phi[c][x, rows, :] = total.astype(BF16)

            def send(i, carry):
                z_copy(c, spare, lax.rem(z + far_first(i), sites), i).start()
                return carry

            lax.fori_loop(0, sites - 1, send, 0)

    def gather_planes(c):
        def arrive(i, carry):
            device = lax.rem(z + i, sites)
            group, valid = group_of(device)

            @pl.when(valid)
            def _():
                z_copy(c, group, device, 0).wait_recv()

            return carry

        lax.fori_loop(1, sites, arrive, 0)
        start_ring(phi_ring, c)

    for op in " ".join(ORDER).split():
        c, step = int(op[1]), int(op[2:] or 0)
        if step > half_ring:
            continue
        if op[0] == "f":
            filter_chunk(c)
        elif op[0] == "F":
            ring_forward(*vectors_ring, c, step)
        elif op[0] == "M":
            multiply(c)
        elif op[0] == "R":
            reduce(c)
        elif op[0] == "Z":
            gather_planes(c)
        else:
            ring_forward(*phi_ring, c, step)
    for c in range(chunks):
        phi_out[c] = phi[c][...]

    for copy in started:
        copy.wait_send()
    for c in range(chunks):

        def sent(i, carry, c=c):
            group, valid = group_of(lax.rem(z + i, sites))

            @pl.when(valid)
            def _():
                partial_copy(c, group, z, z).wait_send()

            return carry

        lax.fori_loop(1, sites, sent, 0)

        @pl.when(reduces)
        def _(c=c):
            def gone(i, carry):
                z_copy(c, spare, z, i).wait_send()
                return carry

            lax.fori_loop(0, sites - 1, gone, 0)


def project(ring, chunks, momenta_count, phi, tau, owner, out, ordered, turned):
    block = chunks * ROWS
    width = ring * block
    piece = ring * ROWS
    for place in range(ring):
        source = 0
        for b in range(ring):
            source = jnp.where(owner[b] == place, b, source)
        for c in range(chunks):
            ordered[:, place * block : (place + 1) * block, c * piece : (c + 1) * piece] = phi[c, source].reshape(
                2 * momenta_count, block, piece
            )
    row = lax.broadcasted_iota(jnp.int32, (width, width), 0)
    spot = lax.broadcasted_iota(jnp.int32, (width, width), 1)
    origin = ((spot % piece) // ROWS) * block + (spot // piece) * ROWS + spot % ROWS
    swap = jnp.where(row == origin, 1.0, 0.0).astype(BF16)
    outer = tau.shape[0]
    for part in range(2):
        rows = tau[:, part].reshape(outer * block, width)
        turned[part] = jnp.dot(rows, swap, preferred_element_type=F32).astype(BF16)
    turned[2] = -turned[1]

    def times(a, p, b):
        return lax.dot_general(turned[a], ordered[2 * p + b], (((1,), (1,)), ((), ())), preferred_element_type=F32)

    for p in range(momenta_count):
        real = times(0, p, 0) + times(2, p, 1)
        out[:, p, 0] = real.astype(BF16).reshape(outer, block, width)
        imag = times(0, p, 1) + times(1, p, 0)
        out[:, p, 1] = imag.astype(BF16).reshape(outer, block, width)


def per_device(eigvecs, links, peramb, block_owner, momenta):
    ring, sites = lax.axis_size("vec"), lax.axis_size("site")
    block = eigvecs.shape[3]
    plane = eigvecs.shape[5]
    chunks = block // ROWS
    momenta_count = momenta.shape[0]
    rows = 2 * momenta_count * block
    groups = max(g for g in range(1, sites + 1) if (rows // ROWS) % g == 0)
    group_rows = rows // groups
    piece = ring * ROWS
    half_ring = ring // 2
    x0 = eigvecs.reshape(6, block // 8, 8, plane)
    table = links.reshape(54, plane)
    vmem = pl.BlockSpec(memory_space=pltpu.VMEM)
    smem = pl.BlockSpec(memory_space=pltpu.SMEM)
    packed = pltpu.VMEM((chunks, 6, ROWS, plane), BF16)
    field = pltpu.VMEM((6, block // 8, 8, plane), F32)
    dma = pltpu.SemaphoreType.DMA
    phi = pl.pallas_call(
        functools.partial(elementals, ring, sites, chunks, momenta_count),
        out_shape=jax.ShapeDtypeStruct((chunks, ring, rows, piece), BF16),
        in_specs=[vmem, vmem, smem, smem],
        out_specs=vmem,
        scratch_shapes=[
            pltpu.VMEM((90, plane), F32),
            pltpu.VMEM((90, 8, plane), F32),
            pltpu.VMEM((momenta_count, 2, 8, plane), F32),
            field,
            field,
            *[packed] * 8,
            pltpu.VMEM((6, rows, plane), BF16),
            *[pltpu.VMEM((ring, 6, ROWS, plane), BF16)] * chunks,
            *[pltpu.VMEM((groups, group_rows, piece), BF16)] * chunks,
            *[pltpu.VMEM((sites, group_rows, piece), BF16)] * chunks,
            *[pltpu.VMEM((ring, rows, piece), BF16)] * chunks,
            dma((2, 2, chunks)),
            dma((2, 2, chunks)),
            dma((2, chunks, half_ring, 2)),
            dma((2, chunks, half_ring, 2)),
            dma((chunks, groups)),
            dma((chunks, sites)),
            dma((chunks, sites)),
            dma((chunks, groups)),
            dma((2, chunks, half_ring, 2)),
            dma((2, chunks, half_ring, 2)),
        ],
        compiler_params=pltpu.CompilerParams(collective_id=0, has_side_effects=True),
        name="elementals",
    )(x0, table, block_owner, momenta)
    sinks, spins = peramb.shape[1], peramb.shape[2]
    width = ring * block
    tau = peramb.reshape(sinks * spins, 2, block, width)
    result = pl.pallas_call(
        functools.partial(project, ring, chunks, momenta_count),
        out_shape=jax.ShapeDtypeStruct((sinks * spins, momenta_count, 2, block, width), BF16),
        in_specs=[vmem, vmem, smem],
        out_specs=vmem,
        scratch_shapes=[
            pltpu.VMEM((2 * momenta_count, width, width), BF16),
            pltpu.VMEM((3, sinks * spins * block, width), BF16),
        ],
        name="project",
    )(phi, tau, block_owner)
    return result.reshape(1, sinks, spins, momenta_count, 2, block, width)


def solution(mesh):
    placed = (
        P(("cfg", "tslice"), None, None, "vec", "site", None),
        P(("cfg", "tslice"), None, None, None, None, "site", None),
        P(("cfg", "tslice"), "site", None, None, "vec", None),
        P(),
        P(),
    )
    return jax.shard_map(
        per_device,
        mesh=mesh,
        in_specs=placed,
        out_specs=P(("cfg", "tslice"), "site", None, None, None, "vec", None),
        check_vma=False,
    )
```

```python
import functools
import math

import jax
import jax.numpy as jnp
from jax import lax
from jax.experimental import pallas as pl
from jax.experimental.pallas import tpu as pltpu
from jax.sharding import PartitionSpec as P

LX = 32
LY = 16
LANES = 128
ROWS = 16
MESH = pl.DeviceIdType.MESH
F32 = jnp.float32
BF16 = jnp.bfloat16

two_pi = 2.0 * math.pi

ORDER = (
    "f0 t2 f1 F01",
    "f2 T F02 F11",
    "F03 F12 F04 F21",
    "M0 F13 F22 F14",
    "M1 F23 R0 F24",
    "M2 R1 Z0 R2",
    "X01 Z1 X02 X11",
    "Z2 X03 X12 X21",
    "X04 O0 X13 X22",
    "X14 O1 X23 X24",
    "O2 P",
)


def link_times(entry, re, im, dagger):
    out_re, out_im = [], []
    for target in range(3):
        total_re = total_im = None
        for source in range(3):
            place = source * 3 + target if dagger else target * 3 + source
            ere, eim = entry[place], entry[9 + place]
            if dagger:
                tre = ere * re[source] + eim * im[source]
                tim = ere * im[source] - eim * re[source]
            else:
                tre = ere * re[source] - eim * im[source]
                tim = ere * im[source] + eim * re[source]
            total_re = tre if total_re is None else total_re + tre
            total_im = tim if total_im is None else total_im + tim
        out_re.append(total_re)
        out_im.append(total_im)
    return out_re + out_im


def elementals(
    ring, sites, chunks, momenta_count,
    x0_hbm, links_hbm, owner_hbm, momenta_hbm, tau_hbm, out_hbm,
    x0, links, owner, momenta, tau, out, ordered, turned, lk, cs, t1, acc, out0, out1, in0, in1, weights, *rest,
):
    gathered, parts, rs_in, phi = (rest[k * chunks : (k + 1) * chunks] for k in range(4))
    loaded, stored, halo_send, halo_recv, f_send, f_recv, rs_send, rs_recv, z_send, z_recv, x_send, x_recv = rest[4 * chunks :]
    x = lax.axis_index("vec")
    z = lax.axis_index("site")
    tiles = links.shape[0] // 54
    plane = tiles * LANES
    block = chunks * ROWS
    half_ring = ring // 2
    groups = parts[0].shape[0]
    group_rows = parts[0].shape[1]

    barrier = pltpu.get_barrier_semaphore()

    def greet(d, carry):
        pl.semaphore_signal(barrier, inc=1, device_id={"site": lax.rem(z + d, sites)}, device_id_type=MESH)
        return carry

    lax.fori_loop(1, sites, greet, 0)
    for d in (1, ring - 1):
        pl.semaphore_signal(barrier, inc=1, device_id={"vec": lax.rem(x + d, ring)}, device_id_type=MESH)

    def lanes_of(t):
        return pl.ds(pl.multiple_of(t * LANES, LANES), LANES)

    def entries(hop, lanes):
        return [lk[hop * 18 + e, :, lanes][None] for e in range(18)]

    def vectors(ref, c, t):
        if ref is x0:
            return [
                x0[pl.ds((comp * block + c * ROWS) * tiles + t, ROWS, stride=tiles), :].reshape(2, 8, LANES)
                for comp in range(6)
            ]
        return [ref[comp, pl.ds(2 * c, 2), :, lanes_of(t)] for comp in range(6)]

    def pack(value):
        return value.reshape(ROWS, LANES).astype(BF16)

    def unpack(value):
        return value.astype(F32).reshape(2, 8, LANES)

    loads = [
        pltpu.make_async_copy(source, target, loaded.at[k])
        for k, (source, target) in enumerate(
            ((links_hbm, links), (x0_hbm, x0), (owner_hbm, owner), (momenta_hbm, momenta), (tau_hbm, tau))
        )
    ]
    for load in loads:
        load.start()

    spread_lane = lax.broadcasted_iota(jnp.int32, (8, LANES), 1)

    def link_row(e, t):
        return jnp.broadcast_to(links[pl.ds(e * tiles + t, 1), :], (8, LANES))

    def spread_in_plane(e, carry):
        for t in range(tiles):
            lanes = pl.ds(t * LANES, LANES)
            along_x, along_y = link_row(e, t), link_row(18 + e, t)
            before = link_row(18 + e, (t + tiles - 1) % tiles)
            lk[e, :, lanes] = along_x
            lk[18 + e, :, lanes] = jnp.where(
                spread_lane % LX == 0, pltpu.roll(along_x, LANES + 1 - LX, 1), pltpu.roll(along_x, 1, 1)
            )
            lk[36 + e, :, lanes] = along_y
            lk[54 + e, :, lanes] = jnp.where(
                spread_lane >= LX, pltpu.roll(along_y, LX, 1), pltpu.roll(before, LX, 1)
            )
        return carry

    def spread_across(e, carry):
        for t in range(tiles):
            lk[72 + e, :, pl.ds(t * LANES, LANES)] = link_row(36 + e, t)
        return carry

    def turn():
        flat = lax.broadcasted_iota(jnp.int32, (8, plane), 1)
        for p in range(momenta_count):
            theta = two_pi * (
                (momenta[p, 0] * (flat % LX)).astype(F32) / LX
                + (momenta[p, 1] * (flat // LX)).astype(F32) / LY
                + (jnp.zeros_like(flat) + momenta[p, 2] * z).astype(F32) / sites
            )
            cs[p, 0] = jnp.cos(theta)
            cs[p, 1] = jnp.sin(theta)

    lane = lax.broadcasted_iota(jnp.int32, (2, 8, LANES), 2)
    last_column = lane % LX == LX - 1
    first_column = lane % LX == 0

    def roll(value, shift):
        return pltpu.roll(value.reshape(ROWS, LANES), shift, 1).reshape(2, 8, LANES)

    def outgoing(source, out, c):
        def body(t, carry):
            lanes = lanes_of(t)
            field = vectors(source, c, t)
            sent = link_times(entries(4, lanes), field[:3], field[3:], True)
            for comp in range(6):
                out[c, 0, comp, :, lanes] = pack(field[comp])
                out[c, 1, comp, :, lanes] = pack(sent[comp])
            return carry

        lax.fori_loop(0, tiles, body, 0)

    def in_plane(source, c):
        def body(t, carry):
            lanes = lanes_of(t)
            field = vectors(source, c, t)
            ahead = [jnp.where(last_column, roll(w, LX - 1), roll(w, LANES - 1)) for w in field]
            total = link_times(entries(0, lanes), ahead[:3], ahead[3:], False)
            behind = [jnp.where(first_column, roll(w, LANES + 1 - LX), roll(w, 1)) for w in field]
            added = link_times(entries(1, lanes), behind[:3], behind[3:], True)
            total = [a + b for a, b in zip(total, added)]
            after = vectors(source, c, lax.rem(t + 1, tiles))
            ahead = [
                jnp.where(lane < LANES - LX, roll(w, LANES - LX), roll(v, LANES - LX)) for w, v in zip(field, after)
            ]
            added = link_times(entries(2, lanes), ahead[:3], ahead[3:], False)
            total = [a + b for a, b in zip(total, added)]
            before = vectors(source, c, lax.rem(t + tiles - 1, tiles))
            behind = [jnp.where(lane >= LX, roll(w, LX), roll(v, LX)) for w, v in zip(field, before)]
            added = link_times(entries(3, lanes), behind[:3], behind[3:], True)
            for comp in range(6):
                acc[comp, pl.ds(2 * c, 2), :, lanes] = total[comp] + added[comp]
            return carry

        lax.fori_loop(0, tiles, body, 0)

    def applied(c, t, arrived):
        lanes = lanes_of(t)
        total = vectors(acc, c, t)
        field = [unpack(arrived[c, 0, comp, :, lanes]) for comp in range(6)]
        added = link_times(entries(4, lanes), field[:3], field[3:], False)
        return [
            (total[comp] + added[comp] + unpack(arrived[c, 1, comp, :, lanes])) * (-1.0 / 6.0) for comp in range(6)
        ]

    up, down = lax.rem(z + 1, sites), lax.rem(z + sites - 1, sites)

    def halo(round_, c, way, target):
        out, arrived = (out0, in0) if round_ == 0 else (out1, in1)
        here, there = (out.at[c], arrived.at[c]) if way is None else (out.at[c, way], arrived.at[c, way])
        return pltpu.make_async_remote_copy(
            src_ref=here, dst_ref=there,
            send_sem=halo_send.at[round_, c], recv_sem=halo_recv.at[round_, c],
            device_id={"site": target}, device_id_type=MESH,
        )

    def send_halo(round_, c):
        halo(round_, c, 0, down).start()
        halo(round_, c, 1, up).start()

    def first_step(c):
        halo(0, c, None, up).wait_recv()

        def first(t, carry):
            lanes = lanes_of(t)
            result = applied(c, t, in0)
            sent = link_times(entries(4, lanes), result[:3], result[3:], True)
            for comp in range(6):
                t1[comp, pl.ds(2 * c, 2), :, lanes] = result[comp]
                out1[c, 0, comp, :, lanes] = pack(result[comp])
                out1[c, 1, comp, :, lanes] = pack(sent[comp])
            return carry

        lax.fori_loop(0, tiles, first, 0)
        send_halo(1, c)

    loads[0].wait()
    lax.fori_loop(0, 18, spread_across, 0)
    loads[1].wait()
    outgoing(x0, out0, 0)
    pl.semaphore_wait(barrier, sites - 1 + 2)
    send_halo(0, 0)
    for c in range(1, chunks):
        outgoing(x0, out0, c)
        if c == 1:
            send_halo(0, c)
    lax.fori_loop(0, 18, spread_in_plane, 0)
    in_plane(x0, 0)
    first_step(0)
    for c in range(2, chunks):
        send_halo(0, c)
    in_plane(t1, 0)
    in_plane(x0, 1)
    first_step(1)
    in_plane(t1, 1)
    in_plane(x0, 2)
    for load in loads[2:]:
        load.wait()
    turn()

    vectors_ring = (gathered, 3, 2, f_send, f_recv)
    phi_ring = (phi, phi[0].shape[1] // 2, 1, x_send, x_recv)

    def ring_copies(which, c, step, source_step):
        buffers, span, pieces, sends, recvs = which
        for piece in range(pieces if step < half_ring else 1):
            for way in range(2):
                if step == half_ring:
                    part = pl.ds(way * span, span)
                elif pieces == 2:
                    part = pl.ds(piece * span, span)
                else:
                    part = pl.ds(0, 2 * span)
                back_by = (ring - source_step) % ring if way == 0 else source_step
                here = buffers[c].at[lax.rem(x + back_by, ring), part]
                yield pltpu.make_async_remote_copy(
                    src_ref=here, dst_ref=here,
                    send_sem=sends.at[c], recv_sem=recvs.at[c, ((step - 1) * pieces + piece) * 2 + way],
                    device_id={"vec": lax.rem(x + (1 if way == 0 else ring - 1), ring)}, device_id_type=MESH,
                )

    def start_ring(which, c):
        for copy in ring_copies(which, c, 1, 0):
            copy.start()

    def ring_forward(which, c, step):
        passed_on = list(ring_copies(which, c, step + 1, step)) if step < half_ring else []
        for number, copy in enumerate(ring_copies(which, c, step, step)):
            copy.wait_recv()
            if step + 1 < half_ring:
                passed_on[number].start()
            elif step < half_ring and which[2] == 2 and number in (0, 3):
                passed_on[number // 2].start()
            elif step < half_ring and which[2] == 1:
                passed_on[number].start()

    def ring_sent(which, c):
        buffers, span, pieces, sends, recvs = which
        whole = buffers[c].at[pl.ds(0, ring - 1)]
        pltpu.make_async_remote_copy(
            src_ref=whole, dst_ref=whole, send_sem=sends.at[c], recv_sem=recvs.at[c, 0],
            device_id={"vec": lax.rem(x + 1, ring)}, device_id_type=MESH,
        ).wait_send()

    def filter_chunk(c):
        halo(1, c, None, up).wait_recv()

        def second(t, carry):
            lanes = lanes_of(t)
            result = applied(c, t, in1)
            start = vectors(x0, c, t)
            for comp in range(6):
                gathered[c][x, comp, :, lanes] = pack(2.0 * result[comp] - start[comp])
            return carry

        lax.fori_loop(0, tiles, second, 0)
        start_ring(vectors_ring, c)

        def phases(t, carry):
            lanes = lanes_of(t)
            for color in range(3):
                re = unpack(gathered[c][x, color, :, lanes])
                im = unpack(gathered[c][x, 3 + color, :, lanes])
                for p in range(momenta_count):
                    cosine, sine = cs[p, 0, :, lanes][None], cs[p, 1, :, lanes][None]
                    shift_re = pack(cosine * re + sine * im)
                    shift_im = pack(cosine * im - sine * re)
                    real = pl.ds(2 * p * block + c * ROWS, ROWS)
                    imag = pl.ds((2 * p + 1) * block + c * ROWS, ROWS)
                    weights[color, real, lanes] = shift_re
                    weights[3 + color, real, lanes] = shift_im
                    weights[color, imag, lanes] = shift_im
                    weights[3 + color, imag, lanes] = -shift_re
            return carry

        lax.fori_loop(0, tiles, phases, 0)

    inverse = []
    for place in range(ring):
        found = 0
        for b in range(ring):
            found = jnp.where(owner[b] == place, b, found)
        inverse.append(found)

    def group_of(device):
        index = (device * groups + sites - 1) // sites
        return index, jnp.logical_and(index < groups, (index * sites) // groups == device)

    my_group, reduces = group_of(z)
    spare = jnp.where(reduces, my_group, 0)

    def far_first(i):
        k = (i + 1) // 2
        return sites // 2 + jnp.where(i % 2 == 0, k, -k)

    def to_plane(c, here, there, send, recv, target):
        return pltpu.make_async_remote_copy(
            src_ref=here, dst_ref=there, send_sem=send.at[c], recv_sem=recv.at[c],
            device_id={"site": target}, device_id_type=MESH,
        )

    def multiply(c):
        total = None
        for comp in range(6):
            left = weights[comp]
            right = jnp.concatenate([gathered[c][inverse[place], comp] for place in range(ring)], axis=0)
            product = lax.dot_general(left, right, (((1,), (1,)), ((), ())), preferred_element_type=F32)
            total = product if total is None else total + product
        parts[c][...] = total.reshape(groups, group_rows, ring * ROWS).astype(BF16)

        def send(i, carry):
            away = far_first(i)
            target = lax.rem(z + away, sites)
            group, valid = group_of(target)

            @pl.when(valid)
            def _():
                to_plane(
                    c, parts[c].at[group], rs_in[c].at[sites - 1 - away], rs_send, rs_recv, target
                ).start()

            return carry

        lax.fori_loop(0, sites - 1, send, 0)

    def rows_of(group, count=1):
        return pl.ds(pl.multiple_of(group * group_rows, ROWS), count * group_rows)

    def reduce(c):
        @pl.when(reduces)
        def _():
            to_plane(c, rs_in[c], rs_in[c], rs_send, rs_recv, up).wait_recv()

            def add(i, total):
                return total + rs_in[c][i].astype(F32)

            total = lax.fori_loop(0, sites - 1, add, parts[c][spare].astype(F32))
            phi[c][x, rows_of(spare), :] = total.astype(BF16)
            mine = phi[c].at[x, rows_of(spare)]

            def send(i, carry):
                to_plane(c, mine, mine, z_send, z_recv, lax.rem(z + far_first(i), sites)).start()
                return carry

            lax.fori_loop(0, sites - 1, send, 0)

    def gather_planes(c):
        @pl.when(reduces)
        def _():
            others = phi[c].at[x, rows_of(0, groups - 1)]
            to_plane(c, others, others, z_send, z_recv, up).wait_recv()

        @pl.when(jnp.logical_not(reduces))
        def _():
            others = phi[c].at[x, rows_of(0, groups)]
            to_plane(c, others, others, z_send, z_recv, up).wait_recv()

        start_ring(phi_ring, c)

    def all_sent(c):
        halo(0, c, None, up).wait_send()
        halo(1, c, None, up).wait_send()
        ring_sent(vectors_ring, c)
        ring_sent(phi_ring, c)

        @pl.when(reduces)
        def _():
            others = parts[c].at[pl.ds(0, groups - 1)]
            to_plane(c, others, others, rs_send, rs_recv, up).wait_send()
            to_plane(c, rs_in[c], rs_in[c], z_send, z_recv, up).wait_send()

        @pl.when(jnp.logical_not(reduces))
        def _():
            to_plane(c, parts[c], parts[c], rs_send, rs_recv, up).wait_send()

    width = ring * block
    piece = ring * ROWS
    outer = tau.shape[0]

    def turn_tau():
        row = lax.broadcasted_iota(jnp.int32, (width, width), 0)
        spot = lax.broadcasted_iota(jnp.int32, (width, width), 1)
        origin = ((spot % piece) // ROWS) * block + (spot // piece) * ROWS + spot % ROWS
        swap = jnp.where(row == origin, 1.0, 0.0).astype(BF16)
        for part in range(2):
            rows = tau[:, part].reshape(outer * block, width)
            turned[part] = jnp.dot(rows, swap, preferred_element_type=F32).astype(BF16)
        turned[2] = -turned[1]

    def order(c):
        for place in range(ring):
            ordered[:, place * block : (place + 1) * block, c * piece : (c + 1) * piece] = phi[c][
                inverse[place]
            ].reshape(2 * momenta_count, block, piece)

    def times(a, p, b):
        return lax.dot_general(turned[a], ordered[2 * p + b], (((1,), (1,)), ((), ())), preferred_element_type=F32)

    def project():
        stores = []
        for p in range(momenta_count):
            real = times(0, p, 0) + times(2, p, 1)
            out[:, p, 0] = real.astype(BF16).reshape(outer, block, width)
            imag = times(0, p, 1) + times(1, p, 0)
            out[:, p, 1] = imag.astype(BF16).reshape(outer, block, width)
            stores.append(pltpu.make_async_copy(out.at[:, p], out_hbm.at[:, p], stored.at[p]))
            stores[p].start()
        for store in stores:
            store.wait()

    for op in " ".join(ORDER).split():
        c, step = int(op[1:2] or 0), int(op[2:] or 0)
        if step > half_ring:
            continue
        if op[0] == "f":
            filter_chunk(c)
        elif op[0] == "T":
            turn_tau()
        elif op[0] == "O":
            order(c)
        elif op[0] == "P":
            project()
        elif op[0] == "t":
            first_step(c)
            in_plane(t1, c)
        elif op[0] == "F":
            ring_forward(vectors_ring, c, step)
        elif op[0] == "M":
            multiply(c)
        elif op[0] == "R":
            reduce(c)
        elif op[0] == "Z":
            gather_planes(c)
        else:
            ring_forward(phi_ring, c, step)
    for c in range(chunks):
        all_sent(c)


def per_device(eigvecs, links, peramb, block_owner, momenta):
    ring, sites = lax.axis_size("vec"), lax.axis_size("site")
    block = eigvecs.shape[3]
    plane = eigvecs.shape[5]
    chunks = block // ROWS
    momenta_count = momenta.shape[0]
    rows = 2 * momenta_count * block
    groups = max(g for g in range(1, sites + 1) if (rows // ROWS) % g == 0)
    group_rows = rows // groups
    piece = ring * ROWS
    half_ring = ring // 2
    x0 = eigvecs.reshape(-1, LANES)
    table = links.reshape(-1, LANES)
    anywhere = pl.BlockSpec(memory_space=pl.ANY)
    packed = pltpu.VMEM((chunks, 2, 6, ROWS, plane), BF16)
    field = pltpu.VMEM((6, block // 8, 8, plane), F32)
    dma = pltpu.SemaphoreType.DMA
    sinks, spins = peramb.shape[1], peramb.shape[2]
    width = ring * block
    tau = peramb.reshape(sinks * spins, 2, block, width)
    out = jax.ShapeDtypeStruct((sinks * spins, momenta_count, 2, block, width), BF16)
    result = pl.pallas_call(
        functools.partial(elementals, ring, sites, chunks, momenta_count),
        out_shape=out,
        in_specs=[anywhere] * 5,
        out_specs=anywhere,
        scratch_shapes=[
            pltpu.VMEM(x0.shape, F32),
            pltpu.VMEM(table.shape, F32),
            pltpu.SMEM(block_owner.shape, jnp.int32),
            pltpu.SMEM(momenta.shape, jnp.int32),
            pltpu.VMEM(tau.shape, BF16),
            pltpu.VMEM(out.shape, BF16),
            pltpu.VMEM((2 * momenta_count, width, width), BF16),
            pltpu.VMEM((3, sinks * spins * block, width), BF16),
            pltpu.VMEM((90, 8, plane), F32),
            pltpu.VMEM((momenta_count, 2, 8, plane), F32),
            field,
            field,
            *[packed] * 4,
            pltpu.VMEM((6, rows, plane), BF16),
            *[pltpu.VMEM((ring, 6, ROWS, plane), BF16)] * chunks,
            *[pltpu.VMEM((groups, group_rows, piece), BF16)] * chunks,
            *[pltpu.VMEM((sites - 1, group_rows, piece), BF16)] * chunks,
            *[pltpu.VMEM((ring, rows, piece), BF16)] * chunks,
            dma((5,)),
            dma((momenta_count,)),
            dma((2, chunks)),
            dma((2, chunks)),
            dma((chunks,)),
            dma((chunks, 4 * half_ring - 2)),
            dma((chunks,)),
            dma((chunks,)),
            dma((chunks,)),
            dma((chunks,)),
            dma((chunks,)),
            dma((chunks, 2 * half_ring)),
        ],
        compiler_params=pltpu.CompilerParams(collective_id=0, has_side_effects=True),
        name="elementals",
    )(x0, table, block_owner, momenta, tau)
    return result.reshape(1, sinks, spins, momenta_count, 2, block, width)


def solution(mesh):
    placed = (
        P(("cfg", "tslice"), None, None, "vec", "site", None),
        P(("cfg", "tslice"), None, None, None, None, "site", None),
        P(("cfg", "tslice"), "site", None, None, "vec", None),
        P(),
        P(),
    )
    return jax.shard_map(
        per_device,
        mesh=mesh,
        in_specs=placed,
        out_specs=P(("cfg", "tslice"), "site", None, None, None, "vec", None),
        check_vma=False,
    )
```
